32 devices in a mesh: seq: 8 (over z, x), mp: 4 (over y, core).
Axes of the slice: x: 2, y: 2, z: 4, core: 2. Of those that a mesh axis runs over, the one named last changes fastest.
Arguments:
- grad_rows: bfloat16 [4096, 8192], P('seq', 'mp'), may hold values from -6 to 6
- img_start: int32 [64], replicated, may hold values from 0 to 4092, as said below
- img_len: int32 [64], replicated, may hold values from 4 to 64, as said below
- img_owner: int32 [64], replicated, may hold values from 0 to 7, as said below
- pre_act: bfloat16 [4096, 5120], P('seq', 'mp'), may hold values from -6 to 6
- w_out: bfloat16 [5120, 8192], P(None, 'mp'), may hold values from -0.0625 to 0.0625
Outputs:
- pre_grad: bfloat16 [4096, 5120], P('seq', 'mp')
- weight_grad: bfloat16 [5120, 8192], P('seq', 'mp')
The draws below stay inside these ranges and needn't reach their ends.
Inputs may be any that keep to these rules, and one draw needn't show every extreme that they name: Image i lies inside positions i * 64 to (i + 1) * 64 - 1: img_start[i] - i * 64 + img_len[i] <= 64. `img_len`: A multiple of 4. In every draw some owner has all its images of exactly 64 merged tokens. `img_owner`: the images i with one value of i % 8 all have different owners, and so do the 8 images of one stripe (images i with one value of i // 8).
All inputs are finite; a program needn't handle non-finite values.
Results may differ from the reference program's by a relative error of at most 0.02.
Values may be sent and summed in bfloat16 or wider, within the bound.
A program may use at most 192 MiB of HBM per device.

```python
import math
import jax
import jax.numpy as jnp
from jax import lax

D_MERGE = 5120
D_OUT = 8192
STRIPE_DEV = 512
FRAME = 64
IMG_STRIPE = 8
NUM_IMG = 64
SEQ_TOT = 4096
N_SEQ = 8


def image_layout(key):
    base = jax.random.fold_in(key, 11)
    subkeys = jax.random.split(base, 4)
    stripes = NUM_IMG // IMG_STRIPE
    image_ids = jnp.arange(NUM_IMG, dtype=jnp.int32)
    lengths = 4 * jax.random.randint(subkeys[0], (NUM_IMG,), 1, FRAME // 4 + 1, dtype=jnp.int32)
    shuffle = jax.random.permutation(subkeys[1], stripes).astype(jnp.int32)
    owners = (shuffle[image_ids // IMG_STRIPE] + image_ids % IMG_STRIPE) % stripes
    chosen = jax.random.randint(subkeys[2], (), 0, stripes, dtype=jnp.int32)
    lengths = jnp.where(owners == chosen, FRAME, lengths).astype(jnp.int32)
    leftover = FRAME - lengths
    offsets = jax.random.randint(subkeys[3], (NUM_IMG,), 0, 1 << 20, dtype=jnp.int32) % (leftover + 1)
    starts = image_ids * FRAME + offsets
    return (starts.astype(jnp.int32), lengths, owners.astype(jnp.int32))


def draw_img_start(key, part):
    return image_layout(key)[0]


def draw_img_len(key, part):
    return image_layout(key)[1]


def draw_img_owner(key, part):
    return image_layout(key)[2]


def spiked(drawn, key, source, target, blocks, factor):
    def block_of(axis_at):
        return (jnp.arange(drawn.shape[axis_at]) // (drawn.shape[axis_at] // blocks)).reshape((-1,) + (1,) * (drawn.ndim - 1 - axis_at))

    one_side = jax.random.permutation(key, blocks)[block_of(target)]
    other_side = (block_of(target) + blocks // 2) % blocks
    return jnp.where((block_of(source) == one_side) | (block_of(source) == other_side), factor * drawn, drawn)


def block_scale(own_key, extent, pieces, low, top_value):
    def one(position, blocks):
        steps = jax.random.uniform(jax.random.fold_in(jax.random.fold_in(own_key, 6), position), (blocks,), jnp.float32, low / len(pieces), top_value / len(pieces))
        return jnp.repeat(jnp.exp(steps), extent[position] // blocks).reshape((-1,) + (1,) * (len(extent) - position - 1))

    level = one(*pieces[0])
    for cut in pieces[1:]:
        level = level * one(*cut)
    return level


def bell_draw(own_key, dims, deviation, limit, shards=(), kind=jnp.bfloat16):
    array = deviation * jax.random.normal(own_key, dims, jnp.float32)
    if shards:
        array = array * block_scale(own_key, dims, shards, -0.22, 0.18)
    return jnp.clip(array, -limit, limit).astype(kind)


def noise_with(key, extent, deviation, most, shards, heavy, kind=jnp.bfloat16):
    drawn = deviation * jax.random.normal(key, extent, jnp.float32)
    if shards:
        drawn = drawn * block_scale(key, extent, shards, -0.22, 0.18)
    return jnp.clip(spiked(drawn, jax.random.fold_in(key, 3), *heavy), -most, most).astype(kind)


def setup_inputs(seed: int = 0) -> dict:
    seeds = jax.random.split(jax.random.key(seed), 7)
    grad_rows = bell_draw(seeds[0], (SEQ_TOT, D_OUT), 1.0, 6.0, ((0, 8), (1, 4)))
    img_start = draw_img_start(jax.random.fold_in(seeds[6], 71), 0)
    img_len = draw_img_len(jax.random.fold_in(seeds[6], 71), 0)
    img_owner = draw_img_owner(jax.random.fold_in(seeds[6], 71), 0)
    pre_act = noise_with(seeds[4], (SEQ_TOT, D_MERGE), 1.0, 6.0, ((0, 8), (1, 4)), (0, 1, 8, 2.0))
    w_out = bell_draw(seeds[5], (D_MERGE, D_OUT), D_OUT ** -0.5, 0.0625, ((1, 4),))
    return dict(grad_rows=grad_rows, img_start=img_start, img_len=img_len, img_owner=img_owner, pre_act=pre_act, w_out=w_out)


def gelu_parts(values):
    normal_cdf = 0.5 * (1.0 + lax.erf(values * 0.7071067811865476))
    density = jnp.exp(-0.5 * values * values) * 0.3989422804014327
    return (values * normal_cdf, normal_cdf + values * density)

def reference(grad_rows, img_start, img_len, img_owner, pre_act, w_out):
    frames = STRIPE_DEV // FRAME
    image_ids = jnp.arange(NUM_IMG, dtype=jnp.int32)
    within = jnp.arange(FRAME, dtype=jnp.int32)
    slot_ids = (img_owner * STRIPE_DEV + image_ids % frames * FRAME)[:, None] + within[None, :]
    positions = jnp.clip(img_start[:, None] + within[None, :], 0, SEQ_TOT - 1).astype(jnp.int32)
    filled = within[None, :] < img_len[:, None]
    picked = jnp.where(filled[:, :, None], grad_rows[positions], jnp.zeros((), jnp.bfloat16))
    routed = jnp.zeros((SEQ_TOT, D_OUT), jnp.bfloat16).at[slot_ids.reshape(-1)].set(picked.reshape(-1, D_OUT))
    hidden_grad = lax.dot_general(routed, w_out, (((1,), (1,)), ((), ())), preferred_element_type=jnp.float32)
    activation, derivative = gelu_parts(pre_act.astype(jnp.float32))
    activation = activation.astype(jnp.bfloat16)
    pre_grad = (hidden_grad * derivative).astype(jnp.bfloat16)
    factor = 1.0 / math.sqrt(SEQ_TOT)

    def accumulate(running, owner_block):
        owner_act, owner_rows = owner_block
        partial_value = lax.dot_general(owner_act, owner_rows, (((0,), (0,)), ((), ())), preferred_element_type=jnp.float32) * factor
        partial_value = lax.optimization_barrier(partial_value.astype(jnp.bfloat16))
        return (running + partial_value.astype(jnp.float32), None)
    weight_grad, _ = lax.scan(accumulate, jnp.zeros((D_MERGE, D_OUT), jnp.float32), (activation.reshape(N_SEQ, STRIPE_DEV, D_MERGE), routed.reshape(N_SEQ, STRIPE_DEV, D_OUT)))
    return (pre_grad, weight_grad.astype(jnp.bfloat16))
```

```python
import functools
import math

import jax
import jax.numpy as jnp
from jax import lax
from jax.experimental import pallas as pl
from jax.experimental.pallas import tpu as pltpu
from jax.sharding import PartitionSpec as P

FRAME = 64
MESH = pl.DeviceIdType.MESH


def gelu_parts(values):
    normal_cdf = 0.5 * (1.0 + lax.erf(values * 0.7071067811865476))
    density = jnp.exp(-0.5 * values * values) * 0.3989422804014327
    return (values * normal_cdf, normal_cdf + values * density)


def exchange_kernel(
    n, mp, inner, pieces,
    rows_ref, act_ref, terms_ref, place_ref,
    rows_out, act_out, hid_out,
    parts, outbuf,
    rs_recv, rs_send, row_recv, row_send, act_recv, act_send, act_fwd, act_own,
    hid_recv, hid_send, local_sem,
):
    s = lax.axis_index("seq")
    m = lax.axis_index("mp")
    outer = n // inner
    z, xi = s // inner, s % inner
    stripe = rows_ref.shape[0]
    piece = stripe // pieces
    half = stripe // 2
    per = act_ref.shape[0]
    xfirst = inner == 2
    seq_peers = [((s + q) % n, m) for q in range(1, n)]
    mp_peers = [(s, (m + q) % mp) for q in range(1, mp)]

    opposite = (m + mp // 2) % mp
    greeted = seq_peers + mp_peers + [((s + q) % n, opposite) for q in range(1, n)]
    barrier = pltpu.get_barrier_semaphore()
    for peer in greeted:
        pl.semaphore_signal(barrier, inc=1, device_id=peer, device_id_type=MESH)
    pl.semaphore_wait(barrier, len(greeted))

    def remote(src, dst, send, recv, peer):
        return pltpu.make_async_remote_copy(
            src_ref=src, dst_ref=dst, send_sem=send, recv_sem=recv,
            device_id=peer, device_id_type=MESH,
        )

    def row_copy(t, p, way, peer, own=False):
        slot = rows_out.at[pl.ds(t * stripe + p * piece, piece)]
        src = rows_ref.at[pl.ds(p * piece, piece)] if own else slot
        return remote(src, slot, row_send.at[t, p, way], row_recv.at[t, p], peer)

    def go(run, copy):
        if run:
            copy.start()
        else:
            copy.wait_send()

    def arrive(run, t, p):
        if run:
            row_copy(t, p, 0, ((s + 1) % n, m)).wait_recv()

    def up(run, t, p, own=False):
        @pl.when(z < outer - 1)
        def _():
            go(run, row_copy(t, p, 0, (s + inner, m), own))

    def down(run, t, p, own=False):
        @pl.when(z > 0)
        def _():
            go(run, row_copy(t, p, 1, (s - inner, m), own))

    def across(run, t, p, own=False):
        for q in range(1, inner):
            go(run, row_copy(t, p, 1 + q, (z * inner + (xi + q) % inner, m), own))

    def loop(first, body):
        def step(p, carry):
            body(p)
            return carry
        lax.fori_loop(first, pieces, step, 0)

    def own_rows(run):
        def body(p):
            up(run, s, p, True)
            down(run, s, p, True)
            across(run, s, p, True)
        loop(0, body)

    def partner_rows(run):
        if xfirst:
            t = z * inner + (1 - xi)
            arrive(run, t, 0)
            up(run, t, 0)
            down(run, t, 0)

    def hop(run, d):
        def one(p, crossing):
            @pl.when(z >= d)
            def _():
                t = s - d * inner
                arrive(run, t, p)
                up(run, t, p)
                if crossing:
                    across(run, t, p)
                else:
                    t2 = (z - d) * inner + (1 - xi)
                    arrive(run, t2, p)
                    up(run, t2, p)

            @pl.when(z + d < outer)
            def _():
                t = s + d * inner
                arrive(run, t, p)
                down(run, t, p)
                if crossing:
                    across(run, t, p)
                else:
                    t2 = (z + d) * inner + (1 - xi)
                    arrive(run, t2, p)
                    down(run, t2, p)

        if xfirst:
            one(0, False)
            loop(1, lambda p: one(p, True))
        else:
            loop(0, lambda p: one(p, True))

    def rest_rows():
        for zz in range(outer):
            for q in range(1, inner):
                t = zz * inner + (xi + q) % inner
                loop(1 if xfirst else 0, lambda p: arrive(True, t, p))

    root_a = s // per
    root_b = (root_a + mp // 2) % mp

    def act_slot(t, h):
        return act_out.at[pl.ds(t * stripe + h * half, half)]

    def act_first(run):
        for j in range(per):
            target = m * per + j

            @pl.when(target != s)
            def _():
                for h, to in ((0, m), (1, opposite)):
                    go(run, remote(
                        act_ref.at[j, pl.ds(h * half, half)], act_slot(s, h),
                        act_send.at[j, h], act_recv.at[s, h], (target, to),
                    ))

            @pl.when(target == s)
            def _():
                for h in range(2):
                    for q, peer in enumerate(mp_peers):
                        go(run, remote(
                            act_ref.at[j, pl.ds(h * half, half)], act_slot(s, h),
                            act_own.at[h, q], act_recv.at[s, h], peer,
                        ))
                mine = pltpu.make_async_copy(
                    act_ref.at[j], act_out.at[pl.ds(s * stripe, stripe)], local_sem.at[1]
                )
                if run:
                    mine.start()
                else:
                    mine.wait()

    def act_wait(t, h):
        remote(act_slot(t, h), act_slot(t, h), act_fwd.at[0, 0], act_recv.at[t, h], mp_peers[0]).wait_recv()

    def act_pass(run):
        for h, root in ((0, root_a), (1, root_b)):
            @pl.when(m == root)
            def _():
                for k in range(1, n):
                    t = (s + k) % n
                    if run:
                        act_wait(t, h)
                    for q, peer in enumerate(mp_peers):
                        go(run, remote(
                            act_slot(t, h), act_slot(t, h), act_fwd.at[t, q], act_recv.at[t, h], peer,
                        ))

    def act_rest():
        for h, root in ((0, root_a), (1, root_b)):
            @pl.when(m != root)
            def _():
                for k in range(1, n):
                    act_wait((s + k) % n, h)

            @pl.when(m != root_a)
            def _():
                act_wait(s, h)

    def sums(run):
        for q, peer in enumerate(mp_peers):
            go(run, remote(terms_ref.at[peer[1]], parts.at[m], rs_send.at[q], rs_recv.at[m], peer))

    def hid_copy(q):
        peer = ((s + q) % n, m)
        return remote(
            outbuf.at[pl.ds(pl.multiple_of(peer[0] * FRAME, FRAME), FRAME)],
            hid_out.at[pl.ds(pl.multiple_of(s * FRAME, FRAME), FRAME)],
            hid_send.at[q], hid_recv.at[s], peer,
        )

    def hid_mine():
        at = pl.ds(pl.multiple_of(s * FRAME, FRAME), FRAME)
        return pltpu.make_async_copy(outbuf.at[at], hid_out.at[at], local_sem.at[2])

    def hidden():
        for q, peer in enumerate(mp_peers):
            remote(terms_ref.at[0], parts.at[peer[1]], rs_send.at[q], rs_recv.at[peer[1]], peer).wait_recv()
        width = parts.shape[2]
        chunk = 256 if width % 256 == 0 else width

        def step(c, carry):
            at = pl.ds(pl.multiple_of(c * chunk, chunk), chunk)
            total = terms_ref[m, :, at].astype(jnp.float32)
            for q in range(1, mp):
                total = total + parts[(m + q) % mp, :, at].astype(jnp.float32)
            outbuf[:, at] = jnp.dot(
                place_ref[...], total.astype(jnp.bfloat16), preferred_element_type=jnp.float32
            ).astype(jnp.bfloat16)
            return carry

        lax.fori_loop(0, width // chunk, step, 0)

    def hid_wait(t):
        at = pl.ds(pl.multiple_of(t * FRAME, FRAME), FRAME)
        remote(outbuf.at[pl.ds(0, FRAME)], hid_out.at[at], hid_send.at[1], hid_recv.at[t], seq_peers[0]).wait_recv()

    keep = pltpu.make_async_copy(rows_ref, rows_out.at[pl.ds(s * stripe, stripe)], local_sem.at[0])
    own_rows(True)
    sums(True)
    act_first(True)
    keep.start()
    partner_rows(True)
    hop(True, 1)
    hidden()
    hop(True, 2)
    for q in range(1, n):
        hid_copy(q).start()
    hid_mine().start()
    act_pass(True)
    for d in range(3, outer):
        hop(True, d)
    rest_rows()
    act_rest()
    for q in range(1, n):
        hid_wait((s + q) % n)

    keep.wait()
    hid_mine().wait()
    own_rows(False)
    sums(False)
    act_first(False)
    partner_rows(False)
    for d in range(1, outer):
        hop(False, d)
    act_pass(False)
    for q in range(1, n):
        hid_copy(q).wait_send()


def exchange(n, mp, rows, acts, terms, place):
    stripe, quarter = rows.shape
    per, _, kept = acts.shape
    width = terms.shape[2]
    inner = n // 4
    pieces = 8 if inner == 2 else 1
    vm = pl.BlockSpec(memory_space=pltpu.VMEM)
    anywhere = pl.BlockSpec(memory_space=pl.ANY)
    dma = pltpu.SemaphoreType.DMA
    return pl.pallas_call(
        functools.partial(exchange_kernel, n, mp, inner, pieces),
        out_shape=(
            jax.ShapeDtypeStruct((n * stripe, quarter), jnp.bfloat16),
            jax.ShapeDtypeStruct((n * stripe, kept), jnp.bfloat16),
            jax.ShapeDtypeStruct((n * FRAME, width), jnp.bfloat16),
        ),
        in_specs=[vm] * 4,
        out_specs=(anywhere,) * 3,
        scratch_shapes=[
            pltpu.VMEM((mp, stripe, width), jnp.bfloat16),
            pltpu.VMEM((n * FRAME, width), jnp.bfloat16),
            dma((mp,)), dma((mp,)),
            dma((n, pieces)), dma((n, pieces, 1 + inner)),
            dma((n, 2)), dma((per, 2)), dma((n, mp)), dma((2, mp)),
            dma((n,)), dma((n,)), dma((3,)),
        ],
        compiler_params=pltpu.CompilerParams(
            collective_id=0, has_side_effects=True, vmem_limit_bytes=60 * 1024 * 1024
        ),
    )(rows, acts, terms, place)


def local(n, mp, grad_rows, img_start, img_len, img_owner, pre_act, w_out):
    stripe, quarter = grad_rows.shape
    width = pre_act.shape[1]
    kept = w_out.shape[0] // n
    frames = stripe // FRAME
    here = lax.axis_index("seq")
    owner = img_owner.reshape(n, frames)
    starts = img_start.reshape(n, frames)
    lengths = img_len.reshape(n, frames)
    row = jnp.arange(FRAME, dtype=jnp.int32)
    image = jnp.arange(n * frames, dtype=jnp.int32).reshape(n, frames)

    mine = (owner == here).astype(jnp.int32)
    offset = jnp.sum(mine * (starts - image * FRAME), axis=0)
    length = jnp.sum(mine * lengths, axis=0)
    token = row[None, :] - offset[:, None]
    token = jnp.where((token >= 0) & (token < length[:, None]), token, -1)
    block = jnp.arange(frames, dtype=jnp.int32)[:, None] * FRAME
    source = jnp.where(token >= 0, block + token, -1).reshape(stripe, 1)
    column = jnp.arange(stripe, dtype=jnp.int32)[None, :]
    shift = (source == column).astype(jnp.bfloat16)

    values = pre_act.astype(jnp.float32)
    activation, derivative = gelu_parts(values)
    activation = activation.astype(jnp.bfloat16)
    shifted = jnp.dot(shift, activation, preferred_element_type=jnp.float32).astype(jnp.bfloat16)
    acts = shifted.reshape(stripe, width // kept, kept).transpose(1, 0, 2)

    my_owner = lax.dynamic_slice_in_dim(owner, here, 1)[0]
    my_start = lax.dynamic_slice_in_dim(starts, here, 1)[0] - here * stripe
    my_length = lax.dynamic_slice_in_dim(lengths, here, 1)[0]
    to = (my_owner[None, :] == jnp.arange(n, dtype=jnp.int32)[:, None]).astype(jnp.int32)
    first = jnp.sum(to * my_start[None, :], axis=1)
    count = jnp.sum(to * my_length[None, :], axis=1)
    at = jnp.where(row[None, :] < count[:, None], first[:, None] + row[None, :], -1)
    place = (at.reshape(n * FRAME, 1) == column).astype(jnp.bfloat16)

    terms = jnp.stack([
        lax.dot_general(
            grad_rows, w_out[q * width:(q + 1) * width], (((1,), (1,)), ((), ())),
            preferred_element_type=jnp.float32,
        ).astype(jnp.bfloat16)
        for q in range(mp)
    ])

    rows_all, act_all, hid = exchange(n, mp, grad_rows, acts, terms, place)

    slot = jnp.arange(stripe, dtype=jnp.int32)
    came = jnp.arange(n * FRAME, dtype=jnp.int32)
    from_me = (owner == here).T
    pick = jnp.repeat(jnp.repeat(from_me, FRAME, axis=0), FRAME, axis=1)
    pick = (pick & (slot[:, None] % FRAME == came[None, :] % FRAME)).astype(jnp.bfloat16)
    hidden_grad = jnp.dot(pick, hid, preferred_element_type=jnp.float32)
    pre_grad = (hidden_grad * derivative).astype(jnp.bfloat16)

    order = (img_owner * frames + jnp.arange(n * frames, dtype=jnp.int32) % frames)
    act_pos = act_all.reshape(n * frames, FRAME, kept)[order].reshape(n * stripe, kept)
    factor = 1.0 / math.sqrt(n * stripe)
    weight_grad = lax.dot_general(
        act_pos, rows_all, (((0,), (0,)), ((), ())), preferred_element_type=jnp.float32
    ) * factor
    return (pre_grad, weight_grad.astype(jnp.bfloat16))


def solution(mesh):
    return jax.shard_map(
        functools.partial(local, mesh.shape["seq"], mesh.shape["mp"]),
        mesh=mesh,
        in_specs=(P("seq", "mp"), P(), P(), P(), P("seq", "mp"), P(None, "mp")),
        out_specs=(P("seq", "mp"), P("seq", "mp")),
        check_vma=False,
    )
```

```python
import functools
import math

import jax
import jax.numpy as jnp
from jax import lax
from jax.experimental import pallas as pl
from jax.experimental.pallas import tpu as pltpu
from jax.sharding import PartitionSpec as P

FRAME = 64
MESH = pl.DeviceIdType.MESH


def gelu_parts(values):
    normal_cdf = 0.5 * (1.0 + lax.erf(values * 0.7071067811865476))
    density = jnp.exp(-0.5 * values * values) * 0.3989422804014327
    return (values * normal_cdf, normal_cdf + values * density)


def exchange_kernel(
    n, mp, inner, pieces,
    rows_ref, act_ref, terms_ref, place_ref,
    rows_out, act_out, hid_out,
    parts, outbuf,
    rs_recv, rs_send, row_recv, row_send, act_recv, act_send, act_fwd, act_own,
    hid_recv, hid_send, local_sem,
):
    s = lax.axis_index("seq")
    m = lax.axis_index("mp")
    outer = n // inner
    z, xi = s // inner, s % inner
    stripe = rows_ref.shape[0]
    piece = stripe // pieces
    tokens = act_ref.shape[1]
    half = tokens // 2
    per = act_ref.shape[0]
    xfirst = inner == 2
    seq_peers = [((s + q) % n, m) for q in range(1, n)]
    mp_peers = [(s, (m + q) % mp) for q in range(1, mp)]

    opposite = (m + mp // 2) % mp
    greeted = seq_peers + mp_peers + [((s + q) % n, opposite) for q in range(1, n)]
    barrier = pltpu.get_barrier_semaphore()
    for peer in greeted:
        pl.semaphore_signal(barrier, inc=1, device_id=peer, device_id_type=MESH)
    pl.semaphore_wait(barrier, len(greeted))

    def remote(src, dst, send, recv, peer):
        return pltpu.make_async_remote_copy(
            src_ref=src, dst_ref=dst, send_sem=send, recv_sem=recv,
            device_id=peer, device_id_type=MESH,
        )

    def row_copy(t, p, way, peer, own=False):
        slot = rows_out.at[pl.ds(t * stripe + p * piece, piece)]
        src = rows_ref.at[pl.ds(p * piece, piece)] if own else slot
        return remote(src, slot, row_send.at[t, p, way], row_recv.at[t, p], peer)

    def go(run, copy):
        if run:
            copy.start()
        else:
            copy.wait_send()

    def arrive(run, t, p):
        if run:
            row_copy(t, p, 0, ((s + 1) % n, m)).wait_recv()

    def up(run, t, p, own=False):
        @pl.when(z < outer - 1)
        def _():
            go(run, row_copy(t, p, 0, (s + inner, m), own))

    def down(run, t, p, own=False):
        @pl.when(z > 0)
        def _():
            go(run, row_copy(t, p, 1, (s - inner, m), own))

    def across(run, t, p, own=False):
        for q in range(1, inner):
            go(run, row_copy(t, p, 1 + q, (z * inner + (xi + q) % inner, m), own))

    def loop(first, body):
        def step(p, carry):
            body(p)
            return carry
        lax.fori_loop(first, pieces, step, 0)

    def own_rows(run):
        def body(p):
            up(run, s, p, True)
            down(run, s, p, True)
            across(run, s, p, True)
        loop(0, body)

    def partner_rows(run):
        if xfirst:
            t = z * inner + (1 - xi)
            arrive(run, t, 0)
            up(run, t, 0)
            down(run, t, 0)

    def hop(run, d):
        def one(p, crossing):
            @pl.when(z >= d)
            def _():
                t = s - d * inner
                arrive(run, t, p)
                up(run, t, p)
                if crossing:
                    across(run, t, p)
                else:
                    t2 = (z - d) * inner + (1 - xi)
                    arrive(run, t2, p)
                    up(run, t2, p)

            @pl.when(z + d < outer)
            def _():
                t = s + d * inner
                arrive(run, t, p)
                down(run, t, p)
                if crossing:
                    across(run, t, p)
                else:
                    t2 = (z + d) * inner + (1 - xi)
                    arrive(run, t2, p)
                    down(run, t2, p)

        if xfirst:
            one(0, False)
            loop(1, lambda p: one(p, True))
        else:
            loop(0, lambda p: one(p, True))

    def rest_rows():
        for zz in range(outer):
            for q in range(1, inner):
                t = zz * inner + (xi + q) % inner
                loop(1 if xfirst else 0, lambda p: arrive(True, t, p))

    root_a = s // per
    root_b = (root_a + mp // 2) % mp

    def act_slot(t, h):
        return act_out.at[pl.ds(t * tokens + h * half, half)]

    def act_first(run):
        for j in range(per):
            target = m * per + j

            @pl.when(target != s)
            def _():
                for h, to in ((0, m), (1, opposite)):
                    go(run, remote(
                        act_ref.at[j, pl.ds(h * half, half)], act_slot(s, h),
                        act_send.at[j, h], act_recv.at[s, h], (target, to),
                    ))

            @pl.when(target == s)
            def _():
                for h in range(2):
                    for q, peer in enumerate(mp_peers):
                        go(run, remote(
                            act_ref.at[j, pl.ds(h * half, half)], act_slot(s, h),
                            act_own.at[h, q], act_recv.at[s, h], peer,
                        ))
                mine = pltpu.make_async_copy(
                    act_ref.at[j], act_out.at[pl.ds(s * tokens, tokens)], local_sem.at[1]
                )
                if run:
                    mine.start()
                else:
                    mine.wait()

    def act_wait(t, h):
        remote(act_slot(t, h), act_slot(t, h), act_fwd.at[0, 0], act_recv.at[t, h], mp_peers[0]).wait_recv()

    def act_pass(run):
        for h, root in ((0, root_a), (1, root_b)):
            @pl.when(m == root)
            def _():
                for k in range(1, n):
                    t = (s + k) % n
                    if run:
                        act_wait(t, h)
                    for q, peer in enumerate(mp_peers):
                        go(run, remote(
                            act_slot(t, h), act_slot(t, h), act_fwd.at[t, q], act_recv.at[t, h], peer,
                        ))

    def act_rest():
        for h, root in ((0, root_a), (1, root_b)):
            @pl.when(m != root)
            def _():
                for k in range(1, n):
                    act_wait((s + k) % n, h)

            @pl.when(m != root_a)
            def _():
                act_wait(s, h)

    def sums(run):
        for q, peer in enumerate(mp_peers):
            go(run, remote(terms_ref.at[peer[1]], parts.at[m], rs_send.at[q], rs_recv.at[m], peer))

    def hid_copy(q):
        peer = ((s + q) % n, m)
        return remote(
            outbuf.at[pl.ds(pl.multiple_of(peer[0] * FRAME, FRAME), FRAME)],
            hid_out.at[pl.ds(pl.multiple_of(s * FRAME, FRAME), FRAME)],
            hid_send.at[q], hid_recv.at[s], peer,
        )

    def hid_mine():
        at = pl.ds(pl.multiple_of(s * FRAME, FRAME), FRAME)
        return pltpu.make_async_copy(outbuf.at[at], hid_out.at[at], local_sem.at[2])

    def hidden():
        for q, peer in enumerate(mp_peers):
            remote(terms_ref.at[0], parts.at[peer[1]], rs_send.at[q], rs_recv.at[peer[1]], peer).wait_recv()
        width = parts.shape[2]
        chunk = 256 if width % 256 == 0 else width

        def step(c, carry):
            at = pl.ds(pl.multiple_of(c * chunk, chunk), chunk)
            total = terms_ref[m, :, at].astype(jnp.float32)
            for q in range(1, mp):
                total = total + parts[(m + q) % mp, :, at].astype(jnp.float32)
            outbuf[:, at] = jnp.dot(
                place_ref[...], total.astype(jnp.bfloat16), preferred_element_type=jnp.float32
            ).astype(jnp.bfloat16)
            return carry

        lax.fori_loop(0, width // chunk, step, 0)

    def hid_wait(t):
        at = pl.ds(pl.multiple_of(t * FRAME, FRAME), FRAME)
        remote(outbuf.at[pl.ds(0, FRAME)], hid_out.at[at], hid_send.at[1], hid_recv.at[t], seq_peers[0]).wait_recv()

    keep = pltpu.make_async_copy(rows_ref, rows_out.at[pl.ds(s * stripe, stripe)], local_sem.at[0])
    act_first(True)
    own_rows(True)
    sums(True)
    keep.start()
    partner_rows(True)
    hop(True, 1)
    act_pass(True)
    hidden()
    hop(True, 2)
    for q in range(1, n):
        hid_copy(q).start()
    hid_mine().start()
    for d in range(3, outer):
        hop(True, d)
    rest_rows()
    act_rest()
    for q in range(1, n):
        hid_wait((s + q) % n)

    keep.wait()
    hid_mine().wait()
    own_rows(False)
    sums(False)
    act_first(False)
    partner_rows(False)
    for d in range(1, outer):
        hop(False, d)
    act_pass(False)
    for q in range(1, n):
        hid_copy(q).wait_send()


def exchange(n, mp, tag, rows, acts, terms, place):
    stripe, quarter = rows.shape
    per, tokens, kept = acts.shape
    width = terms.shape[2]
    inner = n // 4
    pieces = stripe // 32 if inner == 2 else 1
    vm = pl.BlockSpec(memory_space=pltpu.VMEM)
    anywhere = pl.BlockSpec(memory_space=pl.ANY)
    dma = pltpu.SemaphoreType.DMA
    return pl.pallas_call(
        functools.partial(exchange_kernel, n, mp, inner, pieces),
        out_shape=(
            jax.ShapeDtypeStruct((n * stripe, quarter), jnp.bfloat16),
            jax.ShapeDtypeStruct((n * tokens, kept), jnp.bfloat16),
            jax.ShapeDtypeStruct((n * FRAME, width), jnp.bfloat16),
        ),
        in_specs=[vm] * 4,
        out_specs=(anywhere,) * 3,
        scratch_shapes=[
            pltpu.VMEM((mp, stripe, width), jnp.bfloat16),
            pltpu.VMEM((n * FRAME, width), jnp.bfloat16),
            dma((mp,)), dma((mp,)),
            dma((n, pieces)), dma((n, pieces, 1 + inner)),
            dma((n, 2)), dma((per, 2)), dma((n, mp)), dma((2, mp)),
            dma((n,)), dma((n,)), dma((3,)),
        ],
        compiler_params=pltpu.CompilerParams(
            collective_id=tag, has_side_effects=True, vmem_limit_bytes=60 * 1024 * 1024
        ),
    )(rows, acts, terms, place)


def spread(counts, before, base, size):
    r = jnp.arange(size, dtype=jnp.int32)
    inside = (r >= before[..., None]) & (r < (before + counts)[..., None])
    return jnp.sum(jnp.where(inside, (base - before)[..., None] + r + 1, 0), axis=-2) - 1


def local(n, mp, grad_rows, img_start, img_len, img_owner, pre_act, w_out):
    stripe, quarter = grad_rows.shape
    width = pre_act.shape[1]
    kept = w_out.shape[0] // n
    frames = stripe // FRAME
    here = lax.axis_index("seq")
    owner = img_owner.reshape(n, frames)
    starts = img_start.reshape(n, frames)
    lengths = img_len.reshape(n, frames)
    before = jnp.cumsum(lengths, axis=1) - lengths
    row = jnp.arange(FRAME, dtype=jnp.int32)
    column = jnp.arange(stripe, dtype=jnp.int32)

    values = pre_act.astype(jnp.float32)
    activation, derivative = gelu_parts(values)
    activation = activation.astype(jnp.bfloat16)
    acts = activation.reshape(stripe, width // kept, kept).transpose(1, 0, 2)

    my_owner = lax.dynamic_slice_in_dim(owner, here, 1)[0]
    my_start = lax.dynamic_slice_in_dim(starts, here, 1)[0] - here * stripe
    my_length = lax.dynamic_slice_in_dim(lengths, here, 1)[0]
    my_before = lax.dynamic_slice_in_dim(before, here, 1)[0]
    to = (my_owner[None, :] == jnp.arange(n, dtype=jnp.int32)[:, None]).astype(jnp.int32)
    first = jnp.sum(to * my_before[None, :], axis=1)
    count = jnp.sum(to * my_length[None, :], axis=1)
    at = jnp.where(row[None, :] < count[:, None], first[:, None] + row[None, :], -1).reshape(n * FRAME, 1)
    order = img_owner * frames + jnp.arange(n * frames, dtype=jnp.int32) % frames
    factor = 1.0 / math.sqrt(n * stripe)

    def with_size(tag, size, grad_rows, acts, w_out):
        source = spread(my_length, my_before, my_start, size)
        live = (source[:, None] == column[None, :]).astype(jnp.bfloat16)
        rows = jnp.dot(live, grad_rows, preferred_element_type=jnp.float32).astype(jnp.bfloat16)
        place = (at == jnp.arange(size, dtype=jnp.int32)[None, :]).astype(jnp.bfloat16)
        terms = jnp.stack([
            lax.dot_general(
                rows, w_out[q * width:(q + 1) * width], (((1,), (1,)), ((), ())),
                preferred_element_type=jnp.float32,
            ).astype(jnp.bfloat16)
            for q in range(mp)
        ])
        rows_all, act_all, hid = exchange(n, mp, tag, rows, acts, terms, place)
        blocks = act_all.reshape(n * frames, FRAME, kept)[order].reshape(n, stripe, kept)
        block = jnp.broadcast_to(jnp.arange(frames, dtype=jnp.int32) * FRAME, (n, frames))
        taken = spread(lengths, before, block, size)
        lined = (taken[:, :, None] == column[None, None, :]).astype(jnp.bfloat16)
        act_rows = jnp.einsum(
            "trc,tck->trk", lined, blocks, preferred_element_type=jnp.float32
        ).astype(jnp.bfloat16).reshape(n * size, kept)
        product = lax.dot_general(
            act_rows, rows_all, (((0,), (0,)), ((), ())), preferred_element_type=jnp.float32
        ) * factor
        return product.astype(jnp.bfloat16), hid

    sizes = [stripe // 16 * k for k in (12, 13, 16)]
    most = jnp.max(jnp.sum(lengths, axis=1))
    which = sum((most > size).astype(jnp.int32) for size in sizes[:-1])
    weight_grad, hid = lax.switch(
        which,
        [functools.partial(with_size, tag, size) for tag, size in enumerate(sizes)],
        grad_rows, acts, w_out,
    )

    came = jnp.arange(n * FRAME, dtype=jnp.int32)
    from_me = (owner == here).T
    pick = jnp.repeat(jnp.repeat(from_me, FRAME, axis=0), FRAME, axis=1)
    pick = (pick & (column[:, None] % FRAME == came[None, :] % FRAME)).astype(jnp.bfloat16)
    hidden_grad = jnp.dot(pick, hid, preferred_element_type=jnp.float32)
    pre_grad = (hidden_grad * derivative).astype(jnp.bfloat16)
    return (pre_grad, weight_grad)


def solution(mesh):
    return jax.shard_map(
        functools.partial(local, mesh.shape["seq"], mesh.shape["mp"]),
        mesh=mesh,
        in_specs=(P("seq", "mp"), P(), P(), P(), P("seq", "mp"), P(None, "mp")),
        out_specs=(P("seq", "mp"), P("seq", "mp")),
        check_vma=False,
    )
```

```python
import functools
import math

import jax
import jax.numpy as jnp
from jax import lax
from jax.experimental import pallas as pl
from jax.experimental.pallas import tpu as pltpu
from jax.sharding import PartitionSpec as P

FRAME = 64
MESH = pl.DeviceIdType.MESH


def gelu_parts(values):
    normal_cdf = 0.5 * (1.0 + lax.erf(values * 0.7071067811865476))
    density = jnp.exp(-0.5 * values * values) * 0.3989422804014327
    return (values * normal_cdf, normal_cdf + values * density)


def exchange_kernel(
    n, mp, inner, pieces,
    rows_ref, act_ref, place_ref, w_ref,
    rows_out, act_out, hid_out,
    terms_ref, parts, outbuf, w_buf, w_sem,
    rs_recv, rs_send, row_recv, row_send, act_recv, act_send, act_fwd, act_own,
    hid_recv, hid_send, local_sem,
):
    s = lax.axis_index("seq")
    m = lax.axis_index("mp")
    outer = n // inner
    z, xi = s // inner, s % inner
    stripe = rows_ref.shape[0]
    piece = stripe // pieces
    tokens = act_ref.shape[1]
    half = tokens // 2
    per = act_ref.shape[0]
    xfirst = inner == 2
    seq_peers = [((s + q) % n, m) for q in range(1, n)]
    mp_peers = [(s, (m + q) % mp) for q in range(1, mp)]

    opposite = (m + mp // 2) % mp
    greeted = seq_peers + mp_peers + [((s + q) % n, opposite) for q in range(1, n)]
    barrier = pltpu.get_barrier_semaphore()
    for peer in greeted:
        pl.semaphore_signal(barrier, inc=1, device_id=peer, device_id_type=MESH)
    pl.semaphore_wait(barrier, len(greeted))

    def remote(src, dst, send, recv, peer):
        return pltpu.make_async_remote_copy(
            src_ref=src, dst_ref=dst, send_sem=send, recv_sem=recv,
            device_id=peer, device_id_type=MESH,
        )

    def row_copy(t, p, way, peer, own=False):
        slot = rows_out.at[pl.ds(t * stripe + p * piece, piece)]
        src = rows_ref.at[pl.ds(p * piece, piece)] if own else slot
        return remote(src, slot, row_send.at[t, p, way], row_recv.at[t, p], peer)

    def go(run, copy):
        if run:
            copy.start()
        else:
            copy.wait_send()

    def arrive(run, t, p):
        if run:
            row_copy(t, p, 0, ((s + 1) % n, m)).wait_recv()

    def up(run, t, p, own=False):
        @pl.when(z < outer - 1)
        def _():
            go(run, row_copy(t, p, 0, (s + inner, m), own))

    def down(run, t, p, own=False):
        @pl.when(z > 0)
        def _():
            go(run, row_copy(t, p, 1, (s - inner, m), own))

    def across(run, t, p, own=False):
        for q in range(1, inner):
            go(run, row_copy(t, p, 1 + q, (z * inner + (xi + q) % inner, m), own))

    def loop(first, body):
        def step(p, carry):
            body(p)
            return carry
        lax.fori_loop(first, pieces, step, 0)

    def own_rows(run):
        def body(p):
            up(run, s, p, True)
            down(run, s, p, True)
            across(run, s, p, True)
        loop(0, body)

    def partner_rows(run):
        if xfirst:
            t = z * inner + (1 - xi)
            arrive(run, t, 0)
            up(run, t, 0)
            down(run, t, 0)

    def hop(run, d):
        def one(p, crossing):
            @pl.when(z >= d)
            def _():
                t = s - d * inner
                arrive(run, t, p)
                up(run, t, p)
                if crossing:
                    across(run, t, p)
                else:
                    t2 = (z - d) * inner + (1 - xi)
                    arrive(run, t2, p)
                    up(run, t2, p)

            @pl.when(z + d < outer)
            def _():
                t = s + d * inner
                arrive(run, t, p)
                down(run, t, p)
                if crossing:
                    across(run, t, p)
                else:
                    t2 = (z + d) * inner + (1 - xi)
                    arrive(run, t2, p)
                    down(run, t2, p)

        if xfirst:
            one(0, False)
            loop(1, lambda p: one(p, True))
        else:
            loop(0, lambda p: one(p, True))

    def rest_rows():
        for zz in range(outer):
            for q in range(1, inner):
                t = zz * inner + (xi + q) % inner
                loop(1 if xfirst else 0, lambda p: arrive(True, t, p))

    root_a = s // per
    root_b = (root_a + mp // 2) % mp

    def act_slot(t, h):
        return act_out.at[pl.ds(t * tokens + h * half, half)]

    def act_first(run):
        for j in range(per):
            target = m * per + j

            @pl.when(target != s)
            def _():
                for h, to in ((0, m), (1, opposite)):
                    go(run, remote(
                        act_ref.at[j, pl.ds(h * half, half)], act_slot(s, h),
                        act_send.at[j, h], act_recv.at[s, h], (target, to),
                    ))

            @pl.when(target == s)
            def _():
                for h in range(2):
                    for q, peer in enumerate(mp_peers):
                        go(run, remote(
                            act_ref.at[j, pl.ds(h * half, half)], act_slot(s, h),
                            act_own.at[h, q], act_recv.at[s, h], peer,
                        ))
                mine = pltpu.make_async_copy(
                    act_ref.at[j], act_out.at[pl.ds(s * tokens, tokens)], local_sem.at[1]
                )
                if run:
                    mine.start()
                else:
                    mine.wait()

    def act_wait(t, h):
        remote(act_slot(t, h), act_slot(t, h), act_fwd.at[0, 0], act_recv.at[t, h], mp_peers[0]).wait_recv()

    def act_pass(run):
        for h, root in ((0, root_a), (1, root_b)):
            @pl.when(m == root)
            def _():
                for k in range(1, n):
                    t = (s + k) % n
                    if run:
                        act_wait(t, h)
                    for q, peer in enumerate(mp_peers):
                        go(run, remote(
                            act_slot(t, h), act_slot(t, h), act_fwd.at[t, q], act_recv.at[t, h], peer,
                        ))

    def act_rest():
        for h, root in ((0, root_a), (1, root_b)):
            @pl.when(m != root)
            def _():
                for k in range(1, n):
                    act_wait((s + k) % n, h)

            @pl.when(m != root_a)
            def _():
                act_wait(s, h)

    def sums(run):
        for q, peer in enumerate(mp_peers):
            go(run, remote(terms_ref.at[peer[1]], parts.at[m], rs_send.at[q], rs_recv.at[m], peer))

    def hid_copy(q):
        peer = ((s + q) % n, m)
        return remote(
            outbuf.at[pl.ds(pl.multiple_of(peer[0] * FRAME, FRAME), FRAME)],
            hid_out.at[pl.ds(pl.multiple_of(s * FRAME, FRAME), FRAME)],
            hid_send.at[q], hid_recv.at[s], peer,
        )

    def hid_mine():
        at = pl.ds(pl.multiple_of(s * FRAME, FRAME), FRAME)
        return pltpu.make_async_copy(outbuf.at[at], hid_out.at[at], local_sem.at[2])

    def hidden():
        for q, peer in enumerate(mp_peers):
            remote(terms_ref.at[0], parts.at[peer[1]], rs_send.at[q], rs_recv.at[peer[1]], peer).wait_recv()
        width = parts.shape[2]
        chunk = 256 if width % 256 == 0 else width

        def step(c, carry):
            at = pl.ds(pl.multiple_of(c * chunk, chunk), chunk)
            total = terms_ref[m, :, at].astype(jnp.float32)
            for q in range(1, mp):
                total = total + parts[(m + q) % mp, :, at].astype(jnp.float32)
            outbuf[:, at] = jnp.dot(
                place_ref[...], total.astype(jnp.bfloat16), preferred_element_type=jnp.float32
            ).astype(jnp.bfloat16)
            return carry

        lax.fori_loop(0, width // chunk, step, 0)

    def hid_wait(t):
        at = pl.ds(pl.multiple_of(t * FRAME, FRAME), FRAME)
        remote(outbuf.at[pl.ds(0, FRAME)], hid_out.at[at], hid_send.at[1], hid_recv.at[t], seq_peers[0]).wait_recv()

    def multiply():
        width = terms_ref.shape[2]
        tile = w_buf.shape[1]
        per_part = width // tile

        def where(c):
            return (m + 1 + c // per_part) % mp, (c % per_part) * tile

        def fetch(c, slot):
            q, col = where(c)
            at = pl.ds(pl.multiple_of(q * width + col, tile), tile)
            return pltpu.make_async_copy(w_ref.at[at], w_buf.at[slot], w_sem.at[slot])

        count = mp * per_part
        fetch(0, 0).start()

        def step(c, carry):
            slot = c % 2

            @pl.when(c + 1 < count)
            def _():
                fetch(c + 1, 1 - slot).start()
            fetch(c, slot).wait()
            q, col = where(c)
            terms_ref[q, :, pl.ds(pl.multiple_of(col, tile), tile)] = lax.dot_general(
                rows_ref[...], w_buf[slot], (((1,), (1,)), ((), ())),
                preferred_element_type=jnp.float32,
            ).astype(jnp.bfloat16)
            return carry

        lax.fori_loop(0, count, step, 0)

    keep = pltpu.make_async_copy(rows_ref, rows_out.at[pl.ds(s * stripe, stripe)], local_sem.at[0])
    act_first(True)
    own_rows(True)
    keep.start()
    partner_rows(True)
    multiply()
    sums(True)
    hop(True, 1)
    act_pass(True)
    hidden()
    hop(True, 2)
    for q in range(1, n):
        hid_copy(q).start()
    hid_mine().start()
    for d in range(3, outer):
        hop(True, d)
    rest_rows()
    act_rest()
    for q in range(1, n):
        hid_wait((s + q) % n)

    keep.wait()
    hid_mine().wait()
    own_rows(False)
    sums(False)
    act_first(False)
    partner_rows(False)
    for d in range(1, outer):
        hop(False, d)
    act_pass(False)
    for q in range(1, n):
        hid_copy(q).wait_send()


def exchange(n, mp, tag, rows, acts, place, w_out):
    stripe, quarter = rows.shape
    per, tokens, kept = acts.shape
    width = w_out.shape[0] // mp
    inner = n // 4
    pieces = stripe // 32 if inner == 2 else 1
    vm = pl.BlockSpec(memory_space=pltpu.VMEM)
    anywhere = pl.BlockSpec(memory_space=pl.ANY)
    dma = pltpu.SemaphoreType.DMA
    return pl.pallas_call(
        functools.partial(exchange_kernel, n, mp, inner, pieces),
        out_shape=(
            jax.ShapeDtypeStruct((n * stripe, quarter), jnp.bfloat16),
            jax.ShapeDtypeStruct((n * tokens, kept), jnp.bfloat16),
            jax.ShapeDtypeStruct((n * FRAME, width), jnp.bfloat16),
        ),
        in_specs=[vm] * 3 + [anywhere],
        out_specs=(anywhere,) * 3,
        scratch_shapes=[
            pltpu.VMEM((mp, stripe, width), jnp.bfloat16),
            pltpu.VMEM((mp, stripe, width), jnp.bfloat16),
            pltpu.VMEM((n * FRAME, width), jnp.bfloat16),
            pltpu.VMEM((2, 256 if width % 256 == 0 else width, quarter), jnp.bfloat16),
            dma((2,)),
            dma((mp,)), dma((mp,)),
            dma((n, pieces)), dma((n, pieces, 1 + inner)),
            dma((n, 2)), dma((per, 2)), dma((n, mp)), dma((2, mp)),
            dma((n,)), dma((n,)), dma((3,)),
        ],
        compiler_params=pltpu.CompilerParams(
            collective_id=tag, has_side_effects=True, vmem_limit_bytes=60 * 1024 * 1024
        ),
    )(rows, acts, place, w_out)


def spread(counts, before, base, size):
    r = jnp.arange(size, dtype=jnp.int32)
    inside = (r >= before[..., None]) & (r < (before + counts)[..., None])
    return jnp.sum(jnp.where(inside, (base - before)[..., None] + r + 1, 0), axis=-2) - 1


def local(n, mp, grad_rows, img_start, img_len, img_owner, pre_act, w_out):
    stripe, quarter = grad_rows.shape
    width = pre_act.shape[1]
    kept = w_out.shape[0] // n
    frames = stripe // FRAME
    here = lax.axis_index("seq")
    owner = img_owner.reshape(n, frames)
    starts = img_start.reshape(n, frames)
    lengths = img_len.reshape(n, frames)
    before = jnp.cumsum(lengths, axis=1) - lengths
    row = jnp.arange(FRAME, dtype=jnp.int32)
    column = jnp.arange(stripe, dtype=jnp.int32)

    values = pre_act.astype(jnp.float32)
    activation, derivative = gelu_parts(values)
    activation = activation.astype(jnp.bfloat16)
    acts = activation.reshape(stripe, width // kept, kept).transpose(1, 0, 2)

    my_owner = lax.dynamic_slice_in_dim(owner, here, 1)[0]
    my_start = lax.dynamic_slice_in_dim(starts, here, 1)[0] - here * stripe
    my_length = lax.dynamic_slice_in_dim(lengths, here, 1)[0]
    my_before = lax.dynamic_slice_in_dim(before, here, 1)[0]
    to = (my_owner[None, :] == jnp.arange(n, dtype=jnp.int32)[:, None]).astype(jnp.int32)
    first = jnp.sum(to * my_before[None, :], axis=1)
    count = jnp.sum(to * my_length[None, :], axis=1)
    at = jnp.where(row[None, :] < count[:, None], first[:, None] + row[None, :], -1).reshape(n * FRAME, 1)
    order = img_owner * frames + jnp.arange(n * frames, dtype=jnp.int32) % frames
    factor = 1.0 / math.sqrt(n * stripe)

    def with_size(tag, size, grad_rows, acts, w_out):
        source = spread(my_length, my_before, my_start, size)
        live = (source[:, None] == column[None, :]).astype(jnp.bfloat16)
        rows = jnp.dot(live, grad_rows, preferred_element_type=jnp.float32).astype(jnp.bfloat16)
        place = (at == jnp.arange(size, dtype=jnp.int32)[None, :]).astype(jnp.bfloat16)
        rows_all, act_all, hid = exchange(n, mp, tag, rows, acts, place, w_out)
        blocks = act_all.reshape(n * frames, FRAME, kept)[order].reshape(n, stripe, kept)
        block = jnp.broadcast_to(jnp.arange(frames, dtype=jnp.int32) * FRAME, (n, frames))
        taken = spread(lengths, before, block, size)
        lined = (taken[:, :, None] == column[None, None, :]).astype(jnp.bfloat16)
        act_rows = jnp.einsum(
            "trc,tck->trk", lined, blocks, preferred_element_type=jnp.float32
        ).astype(jnp.bfloat16).reshape(n * size, kept)
        product = lax.dot_general(
            act_rows, rows_all, (((0,), (0,)), ((), ())), preferred_element_type=jnp.float32
        ) * factor
        return lax.optimization_barrier(product.astype(jnp.bfloat16)), hid

    sizes = [stripe // 16 * k for k in (12, 13, 16)]
    most = jnp.max(jnp.sum(lengths, axis=1))
    which = sum((most > size).astype(jnp.int32) for size in sizes[:-1])
    weight_grad, hid = lax.switch(
        which,
        [functools.partial(with_size, tag, size) for tag, size in enumerate(sizes)],
        grad_rows, acts, w_out,
    )

    came = jnp.arange(n * FRAME, dtype=jnp.int32)
    from_me = (owner == here).T
    pick = jnp.repeat(jnp.repeat(from_me, FRAME, axis=0), FRAME, axis=1)
    pick = (pick & (column[:, None] % FRAME == came[None, :] % FRAME)).astype(jnp.bfloat16)
    hidden_grad = jnp.dot(pick, hid, preferred_element_type=jnp.float32)
    pre_grad = (hidden_grad * derivative).astype(jnp.bfloat16)
    return (pre_grad, weight_grad)


def solution(mesh):
    return jax.shard_map(
        functools.partial(local, mesh.shape["seq"], mesh.shape["mp"]),
        mesh=mesh,
        in_specs=(P("seq", "mp"), P(), P(), P(), P("seq", "mp"), P(None, "mp")),
        out_specs=(P("seq", "mp"), P("seq", "mp")),
        check_vma=False,
    )
```

```python
import functools
import math

import jax
import jax.numpy as jnp
from jax import lax
from jax.experimental import pallas as pl
from jax.experimental.pallas import tpu as pltpu
from jax.sharding import PartitionSpec as P

FRAME = 64
MESH = pl.DeviceIdType.MESH


def gelu_parts(values):
    normal_cdf = 0.5 * (1.0 + lax.erf(values * 0.7071067811865476))
    density = jnp.exp(-0.5 * values * values) * 0.3989422804014327
    return (values * normal_cdf, normal_cdf + values * density)


def exchange_kernel(
    n, mp, inner, pieces,
    rows_ref, act_ref, place_ref, w_ref,
    rows_out, act_out, hid_out,
    terms_ref, parts, outbuf, w_buf, w_sem,
    rs_recv, rs_send, row_recv, row_send, act_recv, act_send, act_fwd, act_own,
    hid_recv, hid_send, local_sem,
):
    s = lax.axis_index("seq")
    m = lax.axis_index("mp")
    outer = n // inner
    z, xi = s // inner, s % inner
    stripe = rows_ref.shape[0]
    piece = stripe // pieces
    tokens = act_ref.shape[1]
    half = tokens // 2
    per = act_ref.shape[0]
    xfirst = inner == 2
    seq_peers = [((s + q) % n, m) for q in range(1, n)]
    mp_peers = [(s, (m + q) % mp) for q in range(1, mp)]

    opposite = (m + mp // 2) % mp
    greeted = seq_peers + mp_peers + [((s + q) % n, opposite) for q in range(1, n)]
    barrier = pltpu.get_barrier_semaphore()
    for peer in greeted:
        pl.semaphore_signal(barrier, inc=1, device_id=peer, device_id_type=MESH)
    pl.semaphore_wait(barrier, len(greeted))

    def remote(src, dst, send, recv, peer):
        return pltpu.make_async_remote_copy(
            src_ref=src, dst_ref=dst, send_sem=send, recv_sem=recv,
            device_id=peer, device_id_type=MESH,
        )

    def row_copy(t, p, way, peer, own=False):
        slot = rows_out.at[pl.ds(t * stripe + p * piece, piece)]
        src = rows_ref.at[pl.ds(p * piece, piece)] if own else slot
        return remote(src, slot, row_send.at[t, p, way], row_recv.at[t, p], peer)

    def go(run, copy):
        if run:
            copy.start()
        else:
            copy.wait_send()

    def arrive(run, t, p):
        if run:
            row_copy(t, p, 0, ((s + 1) % n, m)).wait_recv()

    def up(run, t, p, own=False):
        @pl.when(z < outer - 1)
        def _():
            go(run, row_copy(t, p, 0, (s + inner, m), own))

    def down(run, t, p, own=False):
        @pl.when(z > 0)
        def _():
            go(run, row_copy(t, p, 1, (s - inner, m), own))

    def across(run, t, p, own=False):
        for q in range(1, inner):
            go(run, row_copy(t, p, 1 + q, (z * inner + (xi + q) % inner, m), own))

    def loop(first, body):
        def step(p, carry):
            body(p)
            return carry
        lax.fori_loop(first, pieces, step, 0)

    def own_rows(run):
        def body(p):
            up(run, s, p, True)
            down(run, s, p, True)
            across(run, s, p, True)
        loop(0, body)

    def partner_rows(run):
        if xfirst:
            t = z * inner + (1 - xi)
            for p in range(2):
                arrive(run, t, p)
                up(run, t, p)
                down(run, t, p)

    def hop(run, d):
        def one(p, crossing):
            @pl.when(z >= d)
            def _():
                t = s - d * inner
                arrive(run, t, p)
                up(run, t, p)
                if crossing:
                    across(run, t, p)
                else:
                    t2 = (z - d) * inner + (1 - xi)
                    arrive(run, t2, p)
                    up(run, t2, p)

            @pl.when(z + d < outer)
            def _():
                t = s + d * inner
                arrive(run, t, p)
                down(run, t, p)
                if crossing:
                    across(run, t, p)
                else:
                    t2 = (z + d) * inner + (1 - xi)
                    arrive(run, t2, p)
                    down(run, t2, p)

        if xfirst:
            one(0, False)
            one(1, False)
            loop(2, lambda p: one(p, True))
        else:
            loop(0, lambda p: one(p, True))

    def rest_rows():
        for zz in range(outer):
            for q in range(1, inner):
                t = zz * inner + (xi + q) % inner
                loop(2 if xfirst else 0, lambda p: arrive(True, t, p))

    root_a = s // per
    root_b = (root_a + mp // 2) % mp

    def act_slot(t, h):
        return act_out.at[pl.ds(t * tokens + h * half, half)]

    def act_first(run):
        for j in range(per):
            target = m * per + j

            @pl.when(target != s)
            def _():
                for h, to in ((0, m), (1, opposite)):
                    go(run, remote(
                        act_ref.at[j, pl.ds(h * half, half)], act_slot(s, h),
                        act_send.at[j, h], act_recv.at[s, h], (target, to),
                    ))

            @pl.when(target == s)
            def _():
                for h in range(2):
                    for q, peer in enumerate(mp_peers):
                        go(run, remote(
                            act_ref.at[j, pl.ds(h * half, half)], act_slot(s, h),
                            act_own.at[h, q], act_recv.at[s, h], peer,
                        ))
                mine = pltpu.make_async_copy(
                    act_ref.at[j], act_out.at[pl.ds(s * tokens, tokens)], local_sem.at[1]
                )
                if run:
                    mine.start()
                else:
                    mine.wait()

    def act_wait(t, h):
        remote(act_slot(t, h), act_slot(t, h), act_fwd.at[0, 0], act_recv.at[t, h], mp_peers[0]).wait_recv()

    def act_pass(run):
        for h, root in ((0, root_a), (1, root_b)):
            @pl.when(m == root)
            def _():
                for k in range(1, n):
                    t = (s + k) % n
                    if run:
                        act_wait(t, h)
                    for q, peer in enumerate(mp_peers):
                        go(run, remote(
                            act_slot(t, h), act_slot(t, h), act_fwd.at[t, q], act_recv.at[t, h], peer,
                        ))

    def act_rest():
        for h, root in ((0, root_a), (1, root_b)):
            @pl.when(m != root)
            def _():
                for k in range(1, n):
                    act_wait((s + k) % n, h)

            @pl.when(m != root_a)
            def _():
                act_wait(s, h)

    def sums(run):
        for q, peer in enumerate(mp_peers):
            go(run, remote(terms_ref.at[peer[1]], parts.at[m], rs_send.at[q], rs_recv.at[m], peer))

    def hid_copy(q):
        peer = ((s + q) % n, m)
        return remote(
            outbuf.at[pl.ds(pl.multiple_of(peer[0] * FRAME, FRAME), FRAME)],
            hid_out.at[pl.ds(pl.multiple_of(s * FRAME, FRAME), FRAME)],
            hid_send.at[q], hid_recv.at[s], peer,
        )

    def hid_mine():
        at = pl.ds(pl.multiple_of(s * FRAME, FRAME), FRAME)
        return pltpu.make_async_copy(outbuf.at[at], hid_out.at[at], local_sem.at[2])

    def hidden():
        for q, peer in enumerate(mp_peers):
            remote(terms_ref.at[0], parts.at[peer[1]], rs_send.at[q], rs_recv.at[peer[1]], peer).wait_recv()
        width = parts.shape[2]
        chunk = 256 if width % 256 == 0 else width

        def step(c, carry):
            at = pl.ds(pl.multiple_of(c * chunk, chunk), chunk)
            total = terms_ref[m, :, at].astype(jnp.float32)
            for q in range(1, mp):
                total = total + parts[(m + q) % mp, :, at].astype(jnp.float32)
            outbuf[:, at] = jnp.dot(
                place_ref[...], total.astype(jnp.bfloat16), preferred_element_type=jnp.float32
            ).astype(jnp.bfloat16)
            return carry

        lax.fori_loop(0, width // chunk, step, 0)

    def hid_wait(t):
        at = pl.ds(pl.multiple_of(t * FRAME, FRAME), FRAME)
        remote(outbuf.at[pl.ds(0, FRAME)], hid_out.at[at], hid_send.at[1], hid_recv.at[t], seq_peers[0]).wait_recv()

    def multiply():
        width = terms_ref.shape[2]
        tile = w_buf.shape[1]
        per_part = width // tile

        def where(c):
            return (m + 1 + c // per_part) % mp, (c % per_part) * tile

        def fetch(c, slot):
            q, col = where(c)
            at = pl.ds(pl.multiple_of(q * width + col, tile), tile)
            return pltpu.make_async_copy(w_ref.at[at], w_buf.at[slot], w_sem.at[slot])

        count = mp * per_part
        fetch(0, 0).start()

        def step(c, carry):
            slot = c % 2

            @pl.when(c + 1 < count)
            def _():
                fetch(c + 1, 1 - slot).start()
            fetch(c, slot).wait()
            q, col = where(c)
            terms_ref[q, :, pl.ds(pl.multiple_of(col, tile), tile)] = lax.dot_general(
                rows_ref[...], w_buf[slot], (((1,), (1,)), ((), ())),
                preferred_element_type=jnp.float32,
            ).astype(jnp.bfloat16)
            return carry

        lax.fori_loop(0, count, step, 0)

    keep = pltpu.make_async_copy(rows_ref, rows_out.at[pl.ds(s * stripe, stripe)], local_sem.at[0])
    act_first(True)
    own_rows(True)
    keep.start()
    partner_rows(True)
    multiply()
    sums(True)
    hop(True, 1)
    act_pass(True)
    hidden()
    hop(True, 2)
    for q in range(1, n):
        hid_copy(q).start()
    hid_mine().start()
    for d in range(3, outer):
        hop(True, d)
    rest_rows()
    act_rest()
    for q in range(1, n):
        hid_wait((s + q) % n)

    keep.wait()
    hid_mine().wait()
    own_rows(False)
    sums(False)
    act_first(False)
    partner_rows(False)
    for d in range(1, outer):
        hop(False, d)
    act_pass(False)
    for q in range(1, n):
        hid_copy(q).wait_send()


def exchange(n, mp, tag, rows, acts, place, w_out):
    stripe, quarter = rows.shape
    per, tokens, kept = acts.shape
    width = w_out.shape[0] // mp
    inner = n // 4
    pieces = stripe // 32 if inner == 2 else 1
    vm = pl.BlockSpec(memory_space=pltpu.VMEM)
    anywhere = pl.BlockSpec(memory_space=pl.ANY)
    dma = pltpu.SemaphoreType.DMA
    return pl.pallas_call(
        functools.partial(exchange_kernel, n, mp, inner, pieces),
        out_shape=(
            jax.ShapeDtypeStruct((n * stripe, quarter), jnp.bfloat16),
            jax.ShapeDtypeStruct((n * tokens, kept), jnp.bfloat16),
            jax.ShapeDtypeStruct((n * FRAME, width), jnp.bfloat16),
        ),
        in_specs=[vm] * 3 + [anywhere],
        out_specs=(anywhere,) * 3,
        scratch_shapes=[
            pltpu.VMEM((mp, stripe, width), jnp.bfloat16),
            pltpu.VMEM((mp, stripe, width), jnp.bfloat16),
            pltpu.VMEM((n * FRAME, width), jnp.bfloat16),
            pltpu.VMEM((2, 256 if width % 256 == 0 else width, quarter), jnp.bfloat16),
            dma((2,)),
            dma((mp,)), dma((mp,)),
            dma((n, pieces)), dma((n, pieces, 1 + inner)),
            dma((n, 2)), dma((per, 2)), dma((n, mp)), dma((2, mp)),
            dma((n,)), dma((n,)), dma((3,)),
        ],
        compiler_params=pltpu.CompilerParams(
            collective_id=tag, has_side_effects=True, vmem_limit_bytes=60 * 1024 * 1024
        ),
    )(rows, acts, place, w_out)


def spread(counts, before, base, size):
    r = jnp.arange(size, dtype=jnp.int32)
    inside = (r >= before[..., None]) & (r < (before + counts)[..., None])
    return jnp.sum(jnp.where(inside, (base - before)[..., None] + r + 1, 0), axis=-2) - 1


def local(n, mp, grad_rows, img_start, img_len, img_owner, pre_act, w_out):
    stripe, quarter = grad_rows.shape
    width = pre_act.shape[1]
    kept = w_out.shape[0] // n
    frames = stripe // FRAME
    here = lax.axis_index("seq")
    owner = img_owner.reshape(n, frames)
    starts = img_start.reshape(n, frames)
    lengths = img_len.reshape(n, frames)
    before = jnp.cumsum(lengths, axis=1) - lengths
    row = jnp.arange(FRAME, dtype=jnp.int32)
    column = jnp.arange(stripe, dtype=jnp.int32)

    values = pre_act.astype(jnp.float32)
    activation, derivative = gelu_parts(values)
    activation = activation.astype(jnp.bfloat16)
    acts = activation.reshape(stripe, width // kept, kept).transpose(1, 0, 2)

    my_owner = lax.dynamic_slice_in_dim(owner, here, 1)[0]
    my_start = lax.dynamic_slice_in_dim(starts, here, 1)[0] - here * stripe
    my_length = lax.dynamic_slice_in_dim(lengths, here, 1)[0]
    my_before = lax.dynamic_slice_in_dim(before, here, 1)[0]
    to = (my_owner[None, :] == jnp.arange(n, dtype=jnp.int32)[:, None]).astype(jnp.int32)
    first = jnp.sum(to * my_before[None, :], axis=1)
    count = jnp.sum(to * my_length[None, :], axis=1)
    at = jnp.where(row[None, :] < count[:, None], first[:, None] + row[None, :], -1).reshape(n * FRAME, 1)
    order = img_owner * frames + jnp.arange(n * frames, dtype=jnp.int32) % frames
    factor = 1.0 / math.sqrt(n * stripe)

    def with_size(tag, size, grad_rows, acts, w_out):
        source = spread(my_length, my_before, my_start, size)
        live = (source[:, None] == column[None, :]).astype(jnp.bfloat16)
        rows = jnp.dot(live, grad_rows, preferred_element_type=jnp.float32).astype(jnp.bfloat16)
        place = (at == jnp.arange(size, dtype=jnp.int32)[None, :]).astype(jnp.bfloat16)
        rows_all, act_all, hid = exchange(n, mp, tag, rows, acts, place, w_out)
        blocks = act_all.reshape(n * frames, FRAME, kept)[order].reshape(n, stripe, kept)
        block = jnp.broadcast_to(jnp.arange(frames, dtype=jnp.int32) * FRAME, (n, frames))
        taken = spread(lengths, before, block, size)
        lined = (taken[:, :, None] == column[None, None, :]).astype(jnp.bfloat16)
        act_rows = jnp.einsum(
            "trc,tck->trk", lined, blocks, preferred_element_type=jnp.float32
        ).astype(jnp.bfloat16).reshape(n * size, kept)
        product = lax.dot_general(
            act_rows, rows_all, (((0,), (0,)), ((), ())), preferred_element_type=jnp.float32
        ) * factor
        return lax.optimization_barrier(product.astype(jnp.bfloat16)), hid

    sizes = [stripe // 16 * k for k in (12, 13, 16)]
    most = jnp.max(jnp.sum(lengths, axis=1))
    which = sum((most > size).astype(jnp.int32) for size in sizes[:-1])
    weight_grad, hid = lax.switch(
        which,
        [functools.partial(with_size, tag, size) for tag, size in enumerate(sizes)],
        grad_rows, acts, w_out,
    )

    came = jnp.arange(n * FRAME, dtype=jnp.int32)
    from_me = (owner == here).T
    pick = jnp.repeat(jnp.repeat(from_me, FRAME, axis=0), FRAME, axis=1)
    pick = (pick & (column[:, None] % FRAME == came[None, :] % FRAME)).astype(jnp.bfloat16)
    hidden_grad = jnp.dot(pick, hid, preferred_element_type=jnp.float32)
    pre_grad = (hidden_grad * derivative).astype(jnp.bfloat16)
    return (pre_grad, weight_grad)


def solution(mesh):
    return jax.shard_map(
        functools.partial(local, mesh.shape["seq"], mesh.shape["mp"]),
        mesh=mesh,
        in_specs=(P("seq", "mp"), P(), P(), P(), P("seq", "mp"), P(None, "mp")),
        out_specs=(P("seq", "mp"), P("seq", "mp")),
        check_vma=False,
    )
```
